256 devices in a mesh: frag: 2 (over y), orb: 128 (over z, x, core).
Axes of the slice: x: 4, y: 2, z: 16, core: 2. Of those that a mesh axis runs over, the one named last changes fastest.
The devices are a block of a 4x16x16 slice.
Arguments:
- slices: float32 [256, 640, 1024], P(('frag', 'orb')), parts along dimension 0, may hold values from -0.5 to 0.5
- occ_energy: float32 [256], P('frag'), parts along dimension 0, may hold values from -2 to -0.5
- virt_energy: float32 [1280], P('frag'), parts along dimension 0, may hold values from 0.3 to 3
- order: int32 [256], P('frag'), parts along dimension 0, may hold values from 0 to 127, each once
- near_keep: int32 [256], P(('frag', 'orb')), parts along dimension 0, may hold values 0 or 1
- far_keep: int32 [128], P('frag'), parts along dimension 0, may hold values 0 or 1
Outputs:
- density: float32 [256, 640, 1024], P(('frag', 'orb')), parts along dimension 0
The draws below stay inside these ranges and needn't reach their ends.
There are 2 independent parts, one for each index of `frag`. The reference program is written for one: setup_inputs(seed, part) draws one part's arguments, and reference() takes and returns one part's arrays. A program takes and returns all parts, laid end to end along the dimension named above; each array names one. Nothing has to cross between parts.
Inputs may be any that keep to these rules, and one draw needn't show every extreme that they name: `order`: each position gets a different energy index.
All inputs are finite; a program needn't handle non-finite values. No bound on the sum of `near_keep` on one device may be relied on, other than what follows from the above.
Results may differ from the reference program's by a relative error of at most 0.0003.
Values sent between devices are 32-bit elements; how exact they have to be, the bound alone decides.
A program may use at most 128 MiB of HBM per device.

```python
import jax
import jax.numpy as jnp
from jax import lax

NV = 640
NAUX = 1024
NOCC = 128


def set_ends(result, rng, smallest, top_value):
    index_at = [jax.random.randint(jax.random.fold_in(rng, axis), (), 0, length) for axis, length in enumerate(result.shape)]
    main_axis = result.shape.index(max(result.shape))
    neighbour = index_at[:main_axis] + [(index_at[main_axis] + 1) % result.shape[main_axis]] + index_at[main_axis + 1:]
    return result.at[tuple(index_at)].set(smallest).at[tuple(neighbour)].set(top_value)


def shard_levels(own_key, dims, cuts, low, largest):
    def one(axis_at, blocks):
        draws = jax.random.uniform(jax.random.fold_in(jax.random.fold_in(own_key, 6), axis_at), (blocks,), jnp.float32, low / len(cuts), largest / len(cuts))
        return jnp.repeat(jnp.exp(draws), dims[axis_at] // blocks).reshape((-1,) + (1,) * (len(dims) - axis_at - 1))

    level = one(*cuts[0])
    for cut in cuts[1:]:
        level = level * one(*cut)
    return level


def normal_values(stream_key, extent, scale, most, shards=(), held_as=jnp.bfloat16):
    result = jax.random.normal(stream_key, extent, jnp.float32) * scale
    if len(shards) > 0:
        result = shard_levels(stream_key, extent, shards, -0.22, 0.18) * result
    return jnp.clip(result, min=-most, max=most).astype(held_as)


def setup_inputs(seed: int = 0, part: int = 0) -> dict:
    key_list = jax.random.split(jax.random.key(seed), 7)
    part_splits = jax.random.split(jax.random.fold_in(key_list[6], part), 7)
    slices = normal_values(part_splits[0], (NOCC, NV, NAUX), 0.08, 0.5, ((0, 128),), jnp.float32)
    occ_energy = jnp.clip(jax.random.uniform(part_splits[1], (NOCC,), jnp.float32, -2.0, -0.5), -2.0, -0.5)
    virt_energy = jnp.clip(jax.random.uniform(part_splits[2], (NV,), jnp.float32, 0.3, 3.0), 0.3, 3.0)
    order = jax.random.permutation(part_splits[3], NOCC).astype(jnp.int32)
    near_keep = set_ends((jax.random.randint(part_splits[4], (NOCC,), 0, 4) < 3).astype(jnp.int32), jax.random.fold_in(part_splits[4], 1), 0, 1)
    far_keep = set_ends((jax.random.randint(part_splits[5], (NOCC // 2,), 0, 4) < 3).astype(jnp.int32), jax.random.fold_in(part_splits[5], 1), 0, 1)
    return {"slices": slices, "occ_energy": occ_energy, "virt_energy": virt_energy, "order": order, "near_keep": near_keep, "far_keep": far_keep}


def amplitudes(left, right, left_energy, right_energy, virtual):
    coupling = lax.dot_general(left, right, (((1,), (1,)), ((), ())), precision=lax.Precision.HIGHEST, preferred_element_type=jnp.float32)
    denom = left_energy + right_energy - virtual[:, None] - virtual[None, :]
    scaled = coupling / denom
    return 2.0 * scaled - scaled.T


def matmul(left, right):
    return jnp.dot(left, right, precision=lax.Precision.HIGHEST, preferred_element_type=jnp.float32)


def reference(slices, occ_energy, virt_energy, order, near_keep, far_keep):
    energy = jnp.take(occ_energy, order)
    middle = NOCC // 2

    def one_orbital(orbital):
        orbital = orbital.astype(jnp.int32)
        next_index = ((orbital + 1) % NOCC).astype(jnp.int32)
        far_index = ((orbital + middle) % NOCC).astype(jnp.int32)
        own = lax.dynamic_index_in_dim(slices, orbital, 0, keepdims=False)
        nearby = lax.dynamic_index_in_dim(slices, next_index, 0, keepdims=False)
        facing = lax.dynamic_index_in_dim(slices, far_index, 0, keepdims=False)
        own_energy = lax.dynamic_index_in_dim(energy, orbital, 0, keepdims=False)
        next_energy = lax.dynamic_index_in_dim(energy, next_index, 0, keepdims=False)
        far_energy = lax.dynamic_index_in_dim(energy, far_index, 0, keepdims=False)
        near_weight = lax.dynamic_index_in_dim(near_keep, orbital, 0, keepdims=False).astype(jnp.float32)
        far_weight = lax.dynamic_index_in_dim(far_keep, (orbital % middle).astype(jnp.int32), 0, keepdims=False).astype(jnp.float32)
        diag_amps = amplitudes(own, own, own_energy, own_energy, virt_energy)
        near_amps = amplitudes(own, nearby, own_energy, next_energy, virt_energy) * near_weight
        far_amps = amplitudes(own, facing, own_energy, far_energy, virt_energy) * far_weight
        mine = matmul(diag_amps, own) + matmul(near_amps, nearby) + matmul(far_amps, facing)
        partner = lax.dot_general(near_amps, own, (((0,), (0,)), ((), ())), precision=lax.Precision.HIGHEST, preferred_element_type=jnp.float32)
        return mine, partner

    mine, partner = lax.map(one_orbital, jnp.arange(NOCC, dtype=jnp.int32))
    return mine + jnp.roll(partner, 1, axis=0)
```

```python
import functools

import jax
import jax.numpy as jnp
from jax import lax
from jax.experimental import pallas as pl
from jax.experimental.pallas import tpu as pltpu
from jax.sharding import PartitionSpec as P

MESH = pl.DeviceIdType.MESH
ROW = 8
CORES = 2
COLS = ROW // CORES
OWN, NEXT, PREV, FAR = range(4)
STEP = 128
TILE = 256
F32 = jnp.float32
BF16 = jnp.bfloat16


def split(x):
    high = x.astype(BF16)
    return high, (x - high.astype(F32)).astype(BF16)


def nt(left, right):
    return lax.dot_general(left, right, (((1,), (1,)), ((), ())), preferred_element_type=F32)


def nn(left, right):
    return jnp.dot(left, right, preferred_element_type=F32)


def kernel(
    n,
    own_ref, occ_ref, virt_ref, order_ref, near_ref, far_ref,
    out_ref,
    transit, held, relay, own_high, own_low, high, low, amp, virt_col, virt_row, weight,
    send_sem, recv_sem, near_send, near_recv, relay_send, relay_recv, weight_sem, load_sem, ready_sem,
):
    rows, depth = out_ref.shape
    rounds = rows // STEP
    half = STEP // 2
    middle = n // 2
    hops = middle // ROW
    quarter = rows // COLS
    me = lax.axis_index("orb")
    inside = lax.rem(me, ROW)
    base = me - inside
    core = lax.rem(inside, CORES)
    col = inside // CORES
    above = lax.rem(me + ROW, n)
    below = lax.rem(me + n - ROW, n)
    after = lax.rem(me + 1, n)
    before = lax.rem(me + n - 1, n)
    opposite = lax.rem(me + middle, n)
    first = inside == 0
    last = inside == ROW - 1

    barrier = pltpu.get_barrier_semaphore()

    def greet(device):
        pl.semaphore_signal(barrier, inc=1, device_id={"orb": device}, device_id_type=MESH)

    load = pltpu.make_async_copy(own_ref, held.at[OWN], load_sem)
    load.start()
    for shift in range(1, ROW):
        greet(base + lax.rem(inside + shift, ROW))
    greet(below)

    @pl.when(first)
    def _():
        greet(before)

    pl.semaphore_wait(barrier, jnp.where(last, ROW + 1, ROW))
    pl.semaphore_signal(ready_sem, inc=1, device_id={"orb": above}, device_id_type=MESH)
    load.wait()
    own = held.at[OWN]

    def remote(src, dst, send, recv, device):
        return pltpu.make_async_remote_copy(
            src_ref=src, dst_ref=dst, send_sem=send, recv_sem=recv,
            device_id={"orb": device}, device_id_type=MESH,
        )

    def lane(part, way):
        return pl.ds(pl.multiple_of(part * STEP + way * half, half), half)

    def start_hop(slot, way):
        hop, part = slot // rounds, lax.rem(slot, rounds)
        target = (above, below)[way]
        at = lane(part, way)
        sems = send_sem.at[slot, way], recv_sem.at[slot, way]

        @pl.when(hop == 0)
        def _():
            remote(own.at[at], transit.at[0, at], *sems, target).start()

        @pl.when((hop > 0) & (hop < hops - 1))
        def _():
            remote(transit.at[hop - 1, at], transit.at[hop, at], *sems, target).start()

        @pl.when(hop == hops - 1)
        def _():
            remote(transit.at[hop - 1, at], held.at[FAR, at], *sems, target).start()

    def far_copy(slot, way):
        at = pl.ds(way * half, half)
        return remote(own.at[at], transit.at[0, at], send_sem.at[slot, way], recv_sem.at[slot, way], above)

    def crossing(src, device):
        return remote(src, relay.at[1], relay_send.at[COLS], relay_recv.at[1], device)

    def to_relay(q, device):
        at = pl.ds(q * quarter, quarter)
        return remote(own.at[at], relay.at[0], relay_send.at[q], relay_recv.at[0], device)

    def near_copy(q, slot, device):
        at = pl.ds(q * quarter, quarter)
        return remote(own.at[at], held.at[slot, at], near_send.at[slot, q], near_recv.at[slot, q], device)

    def weight_copy():
        return remote(weight.at[NEXT], weight.at[PREV], weight_sem.at[0], weight_sem.at[1], after)

    def deliver(slot, device):
        at = pl.ds(pl.multiple_of(col * quarter, quarter), quarter)
        return remote(relay.at[1], held.at[slot, at], relay_send.at[COLS + 1], near_recv.at[slot, col], device)

    @pl.when(last)
    def _():
        crossing(own.at[pl.ds(rows - quarter, quarter)], above).start()
        for q in range(COLS - 1):
            to_relay(q, base + q * CORES + 1).start()

    @pl.when(first)
    def _():
        for q in range(1, COLS):
            to_relay(q, base + q * CORES).start()

    def send_first(way):
        def one(slot, carry):
            start_hop(slot, way)
            return carry

        lax.fori_loop(0, rounds, one, 0)

    send_first(0)

    @pl.when(~last)
    def _():
        for q in range(COLS):
            near_copy(q, PREV, after).start()

    @pl.when(~first)
    def _():
        for q in range(COLS):
            near_copy(q, NEXT, before).start()

    pl.semaphore_wait(ready_sem, 1)

    @pl.when(first)
    def _():
        crossing(own.at[pl.ds(0, quarter)], below).start()

    send_first(1)

    weight[OWN] = jnp.ones(weight.shape[1:], F32)
    weight[NEXT] = jnp.full(weight.shape[1:], near_ref[0].astype(F32), F32)
    weight[FAR] = jnp.full(weight.shape[1:], far_ref[lax.rem(me, middle)].astype(F32), F32)
    virt_row[...] = virt_ref[...].reshape(1, rows)
    virt_col[...] = jnp.broadcast_to(virt_row[...], (STEP, rows)).T

    def prepare(part, carry):
        at = pl.ds(pl.multiple_of(part * STEP, STEP), STEP)
        own_high[at], own_low[at] = split(held[OWN, at])
        high[at] = jnp.zeros((STEP, depth), BF16)
        low[at] = jnp.zeros((STEP, depth), BF16)
        out_ref[at] = jnp.zeros((STEP, depth), F32)
        return carry

    lax.fori_loop(0, rounds, prepare, 0)

    def energy(position):
        return occ_ref[order_ref[position]]

    def compute(which, part):
        at = pl.ds(pl.multiple_of(part * STEP, STEP), STEP)
        partner = jnp.where(which == OWN, me, jnp.where(which == NEXT, after, jnp.where(which == PREV, before, opposite)))
        total = energy(me) + energy(partner)
        w = weight[which, 0:1]
        new_high, new_low = split(held[which, at])
        high[at], low[at] = new_high, new_low
        both = jnp.concatenate([new_high, new_low], axis=0)
        wide = nt(own_high[...], both)
        coupling = wide[:, :STEP] + wide[:, STEP:] + nt(own_low[...], new_high)
        mine = coupling / (total - virt_col[...] - virt_row[:, at])
        amp[:, at] = mine
        row = lax.broadcasted_iota(jnp.int32, (rows, STEP), 0)
        theirs = jnp.where(row < (part + 1) * STEP, amp[at].T, 0.0)
        tilde_high, tilde_low = split(w * (2.0 * mine - theirs))
        tilde_twice = jnp.concatenate([tilde_high, tilde_high], axis=1)
        turned_high, turned_low = split((w * jnp.where(row < part * STEP, mine, 0.0)).T)
        turned = jnp.concatenate([turned_high, turned_low], axis=0)

        def columns(tile, carry):
            over = pl.ds(pl.multiple_of(tile * TILE, TILE), TILE)
            near_high, near_low = high[at, over], low[at, over]
            out_ref[:, over] += nn(tilde_twice, jnp.concatenate([near_high, near_low], axis=0)) + nn(tilde_low, near_high)
            back = nn(turned, high[:, over])
            out_ref[at, over] -= back[:STEP] + back[STEP:] + nn(turned_high, low[:, over])
            return carry

        lax.fori_loop(0, depth // TILE, columns, 0)

    slots = hops * rounds
    own_from, near_from = 3, 18
    near_to = near_from + 2 * rounds

    def step(slot, carry):
        far_copy(slot, 0).wait_recv()
        far_copy(slot, 1).wait_recv()

        @pl.when(slot + rounds < slots)
        def _():
            start_hop(slot + rounds, 0)
            start_hop(slot + rounds, 1)

        @pl.when(slot == 1)
        def _():
            weight_copy().start()

        @pl.when((slot == 2) & ~(first | last))
        def _():
            to_relay(0, above).wait_recv()

            @pl.when(core == 1)
            def _():
                crossing(relay.at[0], above).start()

            @pl.when(core == 0)
            def _():
                crossing(relay.at[0], below).start()

        @pl.when(slot == 9)
        def _():
            crossing(relay.at[0], above).wait_recv()

            @pl.when(core == 1)
            def _():
                deliver(PREV, base).start()

            @pl.when(core == 0)
            def _():
                deliver(NEXT, base + ROW - 1).start()

        @pl.when(slot == near_from)
        def _():
            for q in range(COLS):
                near_copy(q, NEXT, before).wait_recv()

        @pl.when(slot == near_from + rounds)
        def _():
            weight_copy().wait_recv()
            for q in range(COLS):
                near_copy(q, PREV, after).wait_recv()

        early = slot < own_from + rounds
        late = slot >= slots - rounds
        since = slot - near_from

        @pl.when((early & (slot >= own_from)) | ((since >= 0) & (slot < near_to)) | late)
        def _():
            which = jnp.where(early, OWN, jnp.where(late, FAR, NEXT + since // rounds))
            part = jnp.where(early, slot - own_from, jnp.where(late, slot - (slots - rounds), lax.rem(since, rounds)))
            compute(which, part)

        return carry

    lax.fori_loop(0, slots, step, 0)

    def sent(slot, carry):
        far_copy(slot, 0).wait_send()
        far_copy(slot, 1).wait_send()
        return carry

    lax.fori_loop(0, slots, sent, 0)
    weight_copy().wait_send()
    crossing(relay.at[0], above).wait_send()
    deliver(PREV, base).wait_send()

    @pl.when(last)
    def _():
        for q in range(COLS - 1):
            to_relay(q, above).wait_send()

    @pl.when(first)
    def _():
        for q in range(1, COLS):
            to_relay(q, above).wait_send()

    @pl.when(~last)
    def _():
        for q in range(COLS):
            near_copy(q, PREV, after).wait_send()

    @pl.when(~first)
    def _():
        for q in range(COLS):
            near_copy(q, NEXT, before).wait_send()


def body(slices, occ_energy, virt_energy, order, near_keep, far_keep):
    n = lax.axis_size("orb")
    rows, depth = slices.shape[1:]
    hops = n // 2 // ROW
    rounds = rows // STEP
    quarter = rows // COLS
    vmem = pl.BlockSpec(memory_space=pltpu.VMEM)
    smem = pl.BlockSpec(memory_space=pltpu.SMEM)
    dma = pltpu.SemaphoreType.DMA
    density = pl.pallas_call(
        functools.partial(kernel, n),
        out_shape=jax.ShapeDtypeStruct((rows, depth), F32),
        in_specs=[pl.BlockSpec(memory_space=pl.ANY), smem, vmem, smem, smem, smem],
        out_specs=vmem,
        scratch_shapes=[
            pltpu.VMEM((hops - 1, rows, depth), F32),
            pltpu.VMEM((4, rows, depth), F32),
            pltpu.VMEM((2, quarter, depth), F32),
            pltpu.VMEM((rows, depth), BF16),
            pltpu.VMEM((rows, depth), BF16),
            pltpu.VMEM((rows, depth), BF16),
            pltpu.VMEM((rows, depth), BF16),
            pltpu.VMEM((rows, rows), F32),
            pltpu.VMEM((rows, STEP), F32),
            pltpu.VMEM((1, rows), F32),
            pltpu.VMEM((4, 8, STEP), F32),
            dma((hops * rounds, 2)),
            dma((hops * rounds, 2)),
            dma((4, COLS)),
            dma((4, COLS)),
            dma((COLS + 2,)),
            dma((2,)),
            dma((2,)),
            dma,
            pltpu.SemaphoreType.REGULAR,
        ],
        compiler_params=pltpu.CompilerParams(
            collective_id=0, has_side_effects=True, vmem_limit_bytes=62 * 1024 * 1024
        ),
    )(slices[0], occ_energy, virt_energy, order, near_keep, far_keep)
    return density[None]


def solution(mesh):
    return jax.shard_map(
        body,
        mesh=mesh,
        in_specs=(
            P(("frag", "orb"), None, None),
            P("frag"),
            P("frag"),
            P("frag"),
            P(("frag", "orb")),
            P("frag"),
        ),
        out_specs=P(("frag", "orb"), None, None),
        check_vma=False,
    )
```

```python
import functools

import jax
import jax.numpy as jnp
from jax import lax
from jax.experimental import pallas as pl
from jax.experimental.pallas import tpu as pltpu
from jax.sharding import PartitionSpec as P

MESH = pl.DeviceIdType.MESH
ROW = 8
CORES = 2
COLS = ROW // CORES
OWN, NEXT, PREV, FAR = range(4)
STEP = 128
TILE = 256
MOVED = 2
SHIFT = 8
F32 = jnp.float32
BF16 = jnp.bfloat16


def split(x):
    high = x.astype(BF16)
    return high, (x - high.astype(F32)).astype(BF16)


def nt(left, right):
    return lax.dot_general(left, right, (((1,), (1,)), ((), ())), preferred_element_type=F32)


def nn(left, right):
    return jnp.dot(left, right, preferred_element_type=F32)


def kernel(
    n,
    own_ref, occ_ref, virt_ref, order_ref, near_ref, far_ref,
    out_ref,
    transit_up, transit_down, held, relay, own_high, own_low, high, low, amp, virt_col, virt_row, weight,
    send_sem, recv_sem, near_send, near_recv, relay_send, relay_recv, weight_sem, load_sem, ready_sem,
):
    rows, depth = out_ref.shape
    rounds = rows // STEP
    half = STEP // 2
    middle = n // 2
    hops = middle // ROW
    quarter = rows // COLS
    me = lax.axis_index("orb")
    inside = lax.rem(me, ROW)
    base = me - inside
    ring = n // ROW
    place = me // ROW
    core = lax.rem(inside, CORES)
    col = inside // CORES
    above = lax.rem(me + ROW, n)
    below = lax.rem(me + n - ROW, n)
    after = lax.rem(me + 1, n)
    before = lax.rem(me + n - 1, n)
    opposite = lax.rem(me + middle, n)
    first = inside == 0
    last = inside == ROW - 1

    barrier = pltpu.get_barrier_semaphore()

    def greet(device):
        pl.semaphore_signal(barrier, inc=1, device_id={"orb": device}, device_id_type=MESH)

    load = pltpu.make_async_copy(own_ref, held.at[OWN], load_sem)
    load.start()
    for shift in range(1, ROW):
        greet(base + lax.rem(inside + shift, ROW))
    greet(below)

    @pl.when(first)
    def _():
        greet(before)

    pl.semaphore_wait(barrier, jnp.where(last, ROW + 1, ROW))
    pl.semaphore_signal(ready_sem, inc=1, device_id={"orb": above}, device_id_type=MESH)
    load.wait()
    own = held.at[OWN]

    def remote(src, dst, send, recv, device):
        return pltpu.make_async_remote_copy(
            src_ref=src, dst_ref=dst, send_sem=send, recv_sem=recv,
            device_id={"orb": device}, device_id_type=MESH,
        )

    def on_chunk(slot, way, source, act):
        part = lax.rem(slot, rounds)
        moved = (source >= hops) & (part < MOVED)
        for shift in (0, SHIFT):
            size = half - shift if way == 0 else half + shift
            offset = 0 if way == 0 else half - shift
            at = pl.ds(pl.multiple_of(part * STEP + offset, SHIFT), size)
            within = pl.ds(pl.multiple_of(part * (half + way * SHIFT), SHIFT), size)

            @pl.when(moved if shift else ~moved)
            def _():
                act(at, within)

    def source_of(hop, way):
        return lax.rem(place + (ring - hop if way == 0 else hop), ring)

    def start_hop(slot, way):
        hop = slot // rounds
        target = (above, below)[way]
        sems = send_sem.at[slot, way], recv_sem.at[slot, way]

        transit = (transit_up, transit_down)[way]

        def act(at, within):
            @pl.when(hop == 0)
            def _():
                remote(own.at[at], transit.at[0, within], *sems, target).start()

            @pl.when((hop > 0) & (hop < hops - 1))
            def _():
                remote(transit.at[hop - 1, within], transit.at[hop, within], *sems, target).start()

            @pl.when(hop == hops - 1)
            def _():
                remote(transit.at[hop - 1, within], held.at[FAR, at], *sems, target).start()

        on_chunk(slot, way, source_of(hop, way), act)

    def far_copy(slot, way, at):
        sems = send_sem.at[slot, way], recv_sem.at[slot, way]
        return remote(own.at[at], held.at[FAR, at], *sems, above)

    def far_arrived(slot, way):
        on_chunk(slot, way, source_of(slot // rounds + 1, way), lambda at, within: far_copy(slot, way, at).wait_recv())

    def far_sent(slot, way):
        on_chunk(slot, way, source_of(slot // rounds, way), lambda at, within: far_copy(slot, way, at).wait_send())

    def crossing(src, device):
        return remote(src, relay.at[1], relay_send.at[COLS], relay_recv.at[1], device)

    def to_relay(q, device):
        at = pl.ds(q * quarter, quarter)
        return remote(own.at[at], relay.at[0], relay_send.at[q], relay_recv.at[0], device)

    def near_copy(q, slot, device):
        at = pl.ds(q * quarter, quarter)
        return remote(own.at[at], held.at[slot, at], near_send.at[slot, q], near_recv.at[slot, q], device)

    def weight_copy():
        return remote(weight.at[NEXT], weight.at[PREV], weight_sem.at[0], weight_sem.at[1], after)

    def deliver(slot, device):
        at = pl.ds(pl.multiple_of(col * quarter, quarter), quarter)
        return remote(relay.at[1], held.at[slot, at], relay_send.at[COLS + 1], near_recv.at[slot, col], device)

    @pl.when(last)
    def _():
        crossing(own.at[pl.ds(rows - quarter, quarter)], above).start()
        for q in range(COLS - 1):
            to_relay(q, base + q * CORES + 1).start()

    @pl.when(first)
    def _():
        for q in range(1, COLS):
            to_relay(q, base + q * CORES).start()

    def send_first(way):
        def one(slot, carry):
            start_hop(slot, way)
            return carry

        lax.fori_loop(0, rounds, one, 0)

    send_first(0)

    @pl.when(~last)
    def _():
        for q in range(COLS):
            near_copy(q, PREV, after).start()

    @pl.when(~first)
    def _():
        for q in range(COLS):
            near_copy(q, NEXT, before).start()

    pl.semaphore_wait(ready_sem, 1)

    @pl.when(first)
    def _():
        crossing(own.at[pl.ds(0, quarter)], below).start()

    send_first(1)

    weight[OWN] = jnp.ones(weight.shape[1:], F32)
    weight[NEXT] = jnp.full(weight.shape[1:], near_ref[0].astype(F32), F32)
    weight[FAR] = jnp.full(weight.shape[1:], far_ref[lax.rem(me, middle)].astype(F32), F32)
    virt_row[...] = virt_ref[...].reshape(1, rows)
    virt_col[...] = jnp.broadcast_to(virt_row[...], (STEP, rows)).T

    def prepare(part, carry):
        at = pl.ds(pl.multiple_of(part * STEP, STEP), STEP)
        own_high[at], own_low[at] = split(held[OWN, at])
        high[at] = jnp.zeros((STEP, depth), BF16)
        low[at] = jnp.zeros((STEP, depth), BF16)
        out_ref[at] = jnp.zeros((STEP, depth), F32)
        return carry

    lax.fori_loop(0, rounds, prepare, 0)

    def energy(position):
        return occ_ref[order_ref[position]]

    def compute(which, part):
        at = pl.ds(pl.multiple_of(part * STEP, STEP), STEP)
        partner = jnp.where(which == OWN, me, jnp.where(which == NEXT, after, jnp.where(which == PREV, before, opposite)))
        total = energy(me) + energy(partner)
        w = weight[which, 0:1]
        new_high, new_low = split(held[which, at])
        high[at], low[at] = new_high, new_low
        both = jnp.concatenate([new_high, new_low], axis=0)
        wide = nt(own_high[...], both)
        coupling = wide[:, :STEP] + wide[:, STEP:] + nt(own_low[...], new_high)
        mine = coupling / (total - virt_col[...] - virt_row[:, at])
        amp[:, at] = mine
        row = lax.broadcasted_iota(jnp.int32, (rows, STEP), 0)
        theirs = jnp.where(row < (part + 1) * STEP, amp[at].T, 0.0)
        tilde_high, tilde_low = split(w * (2.0 * mine - theirs))
        tilde_twice = jnp.concatenate([tilde_high, tilde_high], axis=1)
        turned_high, turned_low = split((w * jnp.where(row < part * STEP, mine, 0.0)).T)
        turned = jnp.concatenate([turned_high, turned_low], axis=0)

        def columns(tile, carry):
            over = pl.ds(pl.multiple_of(tile * TILE, TILE), TILE)
            near_high, near_low = high[at, over], low[at, over]
            out_ref[:, over] += nn(tilde_twice, jnp.concatenate([near_high, near_low], axis=0)) + nn(tilde_low, near_high)
            back = nn(turned, high[:, over])
            out_ref[at, over] -= back[:STEP] + back[STEP:] + nn(turned_high, low[:, over])
            return carry

        lax.fori_loop(0, depth // TILE, columns, 0)

    slots = hops * rounds
    own_from, deliver_at, near_from = 3, 14, 22
    near_to = near_from + 2 * rounds

    def step(slot, carry):
        for way in range(2):
            far_arrived(slot, way)

            @pl.when(slot + rounds < slots)
            def _():
                start_hop(slot + rounds, way)

        @pl.when(slot == deliver_at)
        def _():
            crossing(relay.at[0], above).wait_recv()

            @pl.when(core == 1)
            def _():
                deliver(PREV, base).start()

            @pl.when(core == 0)
            def _():
                deliver(NEXT, base + ROW - 1).start()

        @pl.when(slot == near_from)
        def _():
            for q in range(COLS):
                near_copy(q, NEXT, before).wait_recv()

        @pl.when(slot == near_from + rounds)
        def _():
            weight_copy().wait_recv()
            for q in range(COLS):
                near_copy(q, PREV, after).wait_recv()

        early = slot < own_from + rounds
        late = slot >= slots - rounds
        since = slot - near_from

        @pl.when((early & (slot >= own_from)) | ((since >= 0) & (slot < near_to)) | late)
        def _():
            which = jnp.where(early, OWN, jnp.where(late, FAR, NEXT + since // rounds))
            part = jnp.where(early, slot - own_from, jnp.where(late, slot - (slots - rounds), lax.rem(since, rounds)))
            compute(which, part)

        return carry

    weight_copy().start()

    @pl.when(~(first | last))
    def _():
        to_relay(0, above).wait_recv()

        @pl.when(core == 1)
        def _():
            crossing(relay.at[0], above).start()

        @pl.when(core == 0)
        def _():
            crossing(relay.at[0], below).start()

    lax.fori_loop(0, slots, step, 0)

    def sent(slot, carry):
        far_sent(slot, 0)
        far_sent(slot, 1)
        return carry

    lax.fori_loop(0, slots, sent, 0)
    weight_copy().wait_send()
    crossing(relay.at[0], above).wait_send()
    deliver(PREV, base).wait_send()

    @pl.when(last)
    def _():
        for q in range(COLS - 1):
            to_relay(q, above).wait_send()

    @pl.when(first)
    def _():
        for q in range(1, COLS):
            to_relay(q, above).wait_send()

    @pl.when(~last)
    def _():
        for q in range(COLS):
            near_copy(q, PREV, after).wait_send()

    @pl.when(~first)
    def _():
        for q in range(COLS):
            near_copy(q, NEXT, before).wait_send()


def body(slices, occ_energy, virt_energy, order, near_keep, far_keep):
    n = lax.axis_size("orb")
    rows, depth = slices.shape[1:]
    hops = n // 2 // ROW
    rounds = rows // STEP
    quarter = rows // COLS
    vmem = pl.BlockSpec(memory_space=pltpu.VMEM)
    smem = pl.BlockSpec(memory_space=pltpu.SMEM)
    dma = pltpu.SemaphoreType.DMA
    density = pl.pallas_call(
        functools.partial(kernel, n),
        out_shape=jax.ShapeDtypeStruct((rows, depth), F32),
        in_specs=[pl.BlockSpec(memory_space=pl.ANY), smem, vmem, smem, smem, smem],
        out_specs=vmem,
        scratch_shapes=[
            pltpu.VMEM((hops - 1, rows // 2, depth), F32),
            pltpu.VMEM((hops - 1, rows // 2 + rounds * SHIFT, depth), F32),
            pltpu.VMEM((4, rows, depth), F32),
            pltpu.VMEM((2, quarter, depth), F32),
            pltpu.VMEM((rows, depth), BF16),
            pltpu.VMEM((rows, depth), BF16),
            pltpu.VMEM((rows, depth), BF16),
            pltpu.VMEM((rows, depth), BF16),
            pltpu.VMEM((rows, rows), F32),
            pltpu.VMEM((rows, STEP), F32),
            pltpu.VMEM((1, rows), F32),
            pltpu.VMEM((4, 8, STEP), F32),
            dma((hops * rounds, 2)),
            dma((hops * rounds, 2)),
            dma((4, COLS)),
            dma((4, COLS)),
            dma((COLS + 2,)),
            dma((2,)),
            dma((2,)),
            dma,
            pltpu.SemaphoreType.REGULAR,
        ],
        compiler_params=pltpu.CompilerParams(
            collective_id=0, has_side_effects=True, vmem_limit_bytes=62 * 1024 * 1024
        ),
    )(slices[0], occ_energy, virt_energy, order, near_keep, far_keep)
    return density[None]


def solution(mesh):
    return jax.shard_map(
        body,
        mesh=mesh,
        in_specs=(
            P(("frag", "orb"), None, None),
            P("frag"),
            P("frag"),
            P("frag"),
            P(("frag", "orb")),
            P("frag"),
        ),
        out_specs=P(("frag", "orb"), None, None),
        check_vma=False,
    )
```

```python
import functools

import jax
import jax.numpy as jnp
from jax import lax
from jax.experimental import pallas as pl
from jax.experimental.pallas import tpu as pltpu
from jax.sharding import PartitionSpec as P

MESH = pl.DeviceIdType.MESH
ROW = 8
CORES = 2
OWN, NEXT, PREV, FAR = range(4)
STEP = 128
TILE = 256
F32 = jnp.float32
BF16 = jnp.bfloat16


def split(x):
    high = x.astype(BF16)
    return high, (x - high.astype(F32)).astype(BF16)


def nt(left, right):
    return lax.dot_general(left, right, (((1,), (1,)), ((), ())), preferred_element_type=F32)


def nn(left, right):
    return jnp.dot(left, right, preferred_element_type=F32)


def kernel(
    n,
    own_ref, occ_ref, virt_ref, order_ref, near_ref, far_ref,
    out_ref,
    transit, held, own_high, own_low, high, low, amp, virt_col, virt_row, weight,
    send_sem, recv_sem, near_send, near_recv, pass_send, weight_sem, load_sem,
):
    rows, depth = out_ref.shape
    rounds = rows // STEP
    middle = n // 2
    hops = middle // ROW
    slots = hops * rounds
    me = lax.axis_index("orb")
    inside = lax.rem(me, ROW)
    base = me - inside
    upward = lax.rem(inside, CORES) == 1
    above = lax.rem(me + ROW, n)
    below = lax.rem(me + n - ROW, n)
    onward = jnp.where(upward, above, below)
    after = lax.rem(me + 1, n)
    before = lax.rem(me + n - 1, n)
    opposite = lax.rem(me + middle, n)
    first = inside == 0
    last = inside == ROW - 1
    row_first, row_last = base, base + ROW - 1

    load = pltpu.make_async_copy(own_ref, held.at[OWN], load_sem)
    load.start()
    barrier = pltpu.get_barrier_semaphore()

    def greet(device):
        pl.semaphore_signal(barrier, inc=1, device_id={"orb": device}, device_id_type=MESH)

    greet(jnp.where(upward, below, above))
    greet(before)
    greet(jnp.where(last, row_first, after))

    @pl.when(first)
    def _():
        greet(row_last)

    pl.semaphore_wait(barrier, jnp.where(last, 4, 3))
    load.wait()
    own = held.at[OWN]

    def remote(src, dst, send, recv, device):
        return pltpu.make_async_remote_copy(
            src_ref=src, dst_ref=dst, send_sem=send, recv_sem=recv,
            device_id={"orb": device}, device_id_type=MESH,
        )

    def band(part):
        return pl.ds(pl.multiple_of(part * STEP, STEP), STEP)

    def start_hop(slot):
        hop, at = slot // rounds, band(lax.rem(slot, rounds))
        sems = send_sem.at[slot], recv_sem.at[slot]

        @pl.when(hop == 0)
        def _():
            remote(own.at[at], transit.at[0, at], *sems, onward).start()

        @pl.when((hop > 0) & (hop < hops - 1))
        def _():
            remote(transit.at[hop - 1, at], transit.at[hop, at], *sems, onward).start()

        @pl.when(hop == hops - 1)
        def _():
            remote(transit.at[hop - 1, at], held.at[FAR, at], *sems, onward).start()

    def far_copy(slot):
        at = pl.ds(0, STEP)
        return remote(own.at[at], transit.at[0, at], send_sem.at[slot], recv_sem.at[slot], onward)

    def near_copy(part, slot, device):
        at = band(part)
        return remote(own.at[at], held.at[slot, at], near_send.at[slot, part], near_recv.at[slot, part], device)

    def pass_copy(part, slot, device):
        at = band(part)
        return remote(transit.at[0, at], held.at[slot, at], pass_send.at[part], near_recv.at[slot, part], device)

    def weight_copy():
        return remote(weight.at[NEXT], weight.at[PREV], weight_sem.at[0], weight_sem.at[1], after)

    def over_parts(act):
        def one(part, carry):
            act(part)
            return carry

        lax.fori_loop(0, rounds, one, 0)

    over_parts(start_hop)

    @pl.when(~last)
    def _():
        over_parts(lambda part: near_copy(part, PREV, after).start())

    @pl.when(~first)
    def _():
        over_parts(lambda part: near_copy(part, NEXT, before).start())

    weight[OWN] = jnp.ones(weight.shape[1:], F32)
    weight[NEXT] = jnp.full(weight.shape[1:], near_ref[0].astype(F32), F32)
    weight[FAR] = jnp.full(weight.shape[1:], far_ref[lax.rem(me, middle)].astype(F32), F32)
    virt_row[...] = virt_ref[...].reshape(1, rows)
    virt_col[...] = jnp.broadcast_to(virt_row[...], (STEP, rows)).T

    def prepare(part, carry):
        at = pl.ds(pl.multiple_of(part * STEP, STEP), STEP)
        own_high[at], own_low[at] = split(held[OWN, at])
        high[at] = jnp.zeros((STEP, depth), BF16)
        low[at] = jnp.zeros((STEP, depth), BF16)
        out_ref[at] = jnp.zeros((STEP, depth), F32)
        return carry

    lax.fori_loop(0, rounds, prepare, 0)

    def energy(position):
        return occ_ref[order_ref[position]]

    def compute(which, part):
        at = pl.ds(pl.multiple_of(part * STEP, STEP), STEP)
        partner = jnp.where(which == OWN, me, jnp.where(which == NEXT, after, jnp.where(which == PREV, before, opposite)))
        total = energy(me) + energy(partner)
        w = weight[which, 0:1]
        new_high, new_low = split(held[which, at])
        high[at], low[at] = new_high, new_low
        both = jnp.concatenate([new_high, new_low], axis=0)
        wide = nt(own_high[...], both)
        coupling = wide[:, :STEP] + wide[:, STEP:] + nt(own_low[...], new_high)
        mine = coupling / (total - virt_col[...] - virt_row[:, at])
        amp[:, at] = mine
        row = lax.broadcasted_iota(jnp.int32, (rows, STEP), 0)
        theirs = jnp.where(row < (part + 1) * STEP, amp[at].T, 0.0)
        tilde_high, tilde_low = split(w * (2.0 * mine - theirs))
        tilde_twice = jnp.concatenate([tilde_high, tilde_high], axis=1)
        turned_high, turned_low = split((w * jnp.where(row < part * STEP, mine, 0.0)).T)
        turned = jnp.concatenate([turned_high, turned_low], axis=0)

        def columns(tile, carry):
            over = pl.ds(pl.multiple_of(tile * TILE, TILE), TILE)
            near_high, near_low = high[at, over], low[at, over]
            out_ref[:, over] += nn(tilde_twice, jnp.concatenate([near_high, near_low], axis=0)) + nn(tilde_low, near_high)
            back = nn(turned, high[:, over])
            out_ref[at, over] -= back[:STEP] + back[STEP:] + nn(turned_high, low[:, over])
            return carry

        lax.fori_loop(0, depth // TILE, columns, 0)

    own_from, near_from = 3, 20
    near_to = near_from + 2 * rounds

    def step(slot, carry):
        far_copy(slot).wait_recv()

        @pl.when(slot + rounds < slots)
        def _():
            start_hop(slot + rounds)

        @pl.when((slot < rounds) & last)
        def _():
            pass_copy(slot, PREV, row_first).start()

        @pl.when((slot < rounds) & first)
        def _():
            pass_copy(slot, NEXT, row_last).start()

        @pl.when(slot == near_from)
        def _():
            over_parts(lambda part: near_copy(part, NEXT, before).wait_recv())

        @pl.when(slot == near_from + rounds)
        def _():
            weight_copy().wait_recv()
            over_parts(lambda part: near_copy(part, PREV, after).wait_recv())

        early = slot < own_from + rounds
        late = slot >= slots - rounds
        since = slot - near_from

        @pl.when((early & (slot >= own_from)) | ((since >= 0) & (slot < near_to)) | late)
        def _():
            which = jnp.where(early, OWN, jnp.where(late, FAR, NEXT + since // rounds))
            part = jnp.where(early, slot - own_from, jnp.where(late, slot - (slots - rounds), lax.rem(since, rounds)))
            compute(which, part)

        return carry

    weight_copy().start()
    lax.fori_loop(0, slots, step, 0)

    def sent(slot, carry):
        far_copy(slot).wait_send()
        return carry

    lax.fori_loop(0, slots, sent, 0)
    weight_copy().wait_send()

    @pl.when(first | last)
    def _():
        over_parts(lambda part: pass_copy(part, PREV, after).wait_send())

    @pl.when(~last)
    def _():
        over_parts(lambda part: near_copy(part, PREV, after).wait_send())

    @pl.when(~first)
    def _():
        over_parts(lambda part: near_copy(part, NEXT, before).wait_send())


def body(slices, occ_energy, virt_energy, order, near_keep, far_keep):
    n = lax.axis_size("orb")
    rows, depth = slices.shape[1:]
    hops = n // 2 // ROW
    rounds = rows // STEP
    vmem = pl.BlockSpec(memory_space=pltpu.VMEM)
    smem = pl.BlockSpec(memory_space=pltpu.SMEM)
    dma = pltpu.SemaphoreType.DMA
    density = pl.pallas_call(
        functools.partial(kernel, n),
        out_shape=jax.ShapeDtypeStruct((rows, depth), F32),
        in_specs=[pl.BlockSpec(memory_space=pl.ANY), smem, vmem, smem, smem, smem],
        out_specs=vmem,
        scratch_shapes=[
            pltpu.VMEM((hops - 1, rows, depth), F32),
            pltpu.VMEM((4, rows, depth), F32),
            pltpu.VMEM((rows, depth), BF16),
            pltpu.VMEM((rows, depth), BF16),
            pltpu.VMEM((rows, depth), BF16),
            pltpu.VMEM((rows, depth), BF16),
            pltpu.VMEM((rows, rows), F32),
            pltpu.VMEM((rows, STEP), F32),
            pltpu.VMEM((1, rows), F32),
            pltpu.VMEM((4, 8, STEP), F32),
            dma((hops * rounds,)),
            dma((hops * rounds,)),
            dma((4, rounds)),
            dma((4, rounds)),
            dma((rounds,)),
            dma((2,)),
            dma,
        ],
        compiler_params=pltpu.CompilerParams(
            collective_id=0, has_side_effects=True, vmem_limit_bytes=62 * 1024 * 1024
        ),
    )(slices[0], occ_energy, virt_energy, order, near_keep, far_keep)
    return density[None]


def solution(mesh):
    return jax.shard_map(
        body,
        mesh=mesh,
        in_specs=(
            P(("frag", "orb"), None, None),
            P("frag"),
            P("frag"),
            P("frag"),
            P(("frag", "orb")),
            P("frag"),
        ),
        out_specs=P(("frag", "orb"), None, None),
        check_vma=False,
    )
```

```python
import functools

import jax
import jax.numpy as jnp
from jax import lax
from jax.experimental import pallas as pl
from jax.experimental.pallas import tpu as pltpu
from jax.sharding import PartitionSpec as P

MESH = pl.DeviceIdType.MESH
ROW = 8
CORES = 2
OWN, NEXT, PREV, FAR = range(4)
STEP = 128
TILE = 256
MINOR = 24
F32 = jnp.float32
BF16 = jnp.bfloat16


def split(x):
    high = x.astype(BF16)
    return high, (x - high.astype(F32)).astype(BF16)


def nt(left, right):
    return lax.dot_general(left, right, (((1,), (1,)), ((), ())), preferred_element_type=F32)


def nn(left, right):
    return jnp.dot(left, right, preferred_element_type=F32)


def kernel(
    n,
    own_ref, occ_ref, virt_ref, order_ref, near_ref, far_ref,
    out_ref,
    transit, minor, held, own_high, own_low, high, low, amp, virt_col, virt_row, weight,
    send_sem, recv_sem, minor_send, minor_recv, near_send, near_recv, pass_send, weight_sem, load_sem,
):
    rows, depth = out_ref.shape
    rounds = rows // STEP
    middle = n // 2
    hops = middle // ROW
    slots = hops * rounds
    me = lax.axis_index("orb")
    inside = lax.rem(me, ROW)
    base = me - inside
    upward = lax.rem(inside, CORES) == 1
    above = lax.rem(me + ROW, n)
    below = lax.rem(me + n - ROW, n)
    onward = jnp.where(upward, above, below)
    feeder = jnp.where(upward, below, above)
    ring = n // ROW
    place = me // ROW
    after = lax.rem(me + 1, n)
    before = lax.rem(me + n - 1, n)
    opposite = lax.rem(me + middle, n)
    first = inside == 0
    last = inside == ROW - 1
    row_first, row_last = base, base + ROW - 1

    load = pltpu.make_async_copy(own_ref, held.at[OWN], load_sem)
    load.start()
    barrier = pltpu.get_barrier_semaphore()

    def greet(device):
        pl.semaphore_signal(barrier, inc=1, device_id={"orb": device}, device_id_type=MESH)

    greet(feeder)

    @pl.when(upward)
    def _():
        greet(before)
        greet(jnp.where(last, row_first, after))

    @pl.when(first)
    def _():
        greet(before)

    pl.semaphore_wait(barrier, jnp.where(upward, jnp.where(last, 2, 1), 3))
    load.wait()
    own = held.at[OWN]

    def remote(src, dst, send, recv, device):
        return pltpu.make_async_remote_copy(
            src_ref=src, dst_ref=dst, send_sem=send, recv_sem=recv,
            device_id={"orb": device}, device_id_type=MESH,
        )

    def band(part):
        return pl.ds(pl.multiple_of(part * STEP, STEP), STEP)

    def moved(source):
        return (source >= hops) == upward

    def from_feeder(distance):
        return lax.rem(place + jnp.where(upward, ring - distance, distance), ring)

    def to_feeder(distance):
        return lax.rem(place + jnp.where(upward, distance, ring - distance), ring)

    def on_chunk(hop, part, source, act):
        short = (hop > 0) & (part == 0) & moved(source)

        @pl.when(short)
        def _():
            act(pl.ds(MINOR, STEP - MINOR))

        @pl.when(~short)
        def _():
            act(band(part))

    def start_hop(slot):
        hop, part = slot // rounds, lax.rem(slot, rounds)
        sems = send_sem.at[slot], recv_sem.at[slot]

        def act(at):
            @pl.when(hop == 0)
            def _():
                remote(own.at[at], transit.at[0, at], *sems, onward).start()

            @pl.when((hop > 0) & (hop < hops - 1))
            def _():
                remote(transit.at[hop - 1, at], transit.at[hop, at], *sems, onward).start()

            @pl.when(hop == hops - 1)
            def _():
                remote(transit.at[hop - 1, at], held.at[FAR, at], *sems, onward).start()

        on_chunk(hop, part, from_feeder(hop), act)

    def far_copy(slot, at):
        return remote(own.at[at], transit.at[0, at], send_sem.at[slot], recv_sem.at[slot], onward)

    def far_arrived(slot):
        hop, part = slot // rounds, lax.rem(slot, rounds)
        on_chunk(hop, part, from_feeder(hop + 1), lambda at: far_copy(slot, at).wait_recv())

    def far_sent(slot):
        hop, part = slot // rounds, lax.rem(slot, rounds)
        on_chunk(hop, part, from_feeder(hop), lambda at: far_copy(slot, at).wait_send())

    few = pl.ds(0, MINOR)

    def minor_copy(hop, src, dst):
        return remote(src, dst, minor_send.at[hop], minor_recv.at[hop], feeder)

    def minor_any(hop):
        return minor_copy(hop, own.at[few], held.at[FAR, few])

    def minor_hop(hop):
        @pl.when(moved(to_feeder(hop)))
        def _():
            @pl.when(hop == 0)
            def _():
                minor_copy(hop, own.at[few], minor.at[0]).start()

            @pl.when(hop > 0)
            def _():
                minor_any(hop - 1).wait_recv()

            @pl.when((hop > 0) & (hop < hops - 1))
            def _():
                minor_copy(hop, minor.at[hop - 1], minor.at[hop]).start()

            @pl.when(hop == hops - 1)
            def _():
                minor_copy(hop, minor.at[hop - 1], held.at[FAR, few]).start()

    def near_copy(part, slot, device):
        at = band(part)
        return remote(own.at[at], held.at[slot, at], near_send.at[slot, part], near_recv.at[slot, part], device)

    def pass_copy(part, slot, device):
        at = band(part)
        return remote(transit.at[0, at], held.at[slot, at], pass_send.at[part], near_recv.at[slot, part], device)

    def weight_copy():
        return remote(weight.at[NEXT], weight.at[PREV], weight_sem.at[0], weight_sem.at[1], after)

    def over_parts(act):
        def one(part, carry):
            act(part)
            return carry

        lax.fori_loop(0, rounds, one, 0)

    over_parts(start_hop)

    @pl.when(~upward)
    def _():
        over_parts(lambda part: near_copy(part, PREV, after).start())

        @pl.when(~first)
        def _():
            over_parts(lambda part: near_copy(part, NEXT, before).start())

    weight[OWN] = jnp.ones(weight.shape[1:], F32)
    weight[NEXT] = jnp.full(weight.shape[1:], near_ref[0].astype(F32), F32)
    weight[FAR] = jnp.full(weight.shape[1:], far_ref[lax.rem(me, middle)].astype(F32), F32)
    virt_row[...] = virt_ref[...].reshape(1, rows)
    virt_col[...] = jnp.broadcast_to(virt_row[...], (STEP, rows)).T

    def prepare(part, carry):
        at = pl.ds(pl.multiple_of(part * STEP, STEP), STEP)
        own_high[at], own_low[at] = split(held[OWN, at])
        high[at] = jnp.zeros((STEP, depth), BF16)
        low[at] = jnp.zeros((STEP, depth), BF16)
        out_ref[at] = jnp.zeros((STEP, depth), F32)
        return carry

    lax.fori_loop(0, rounds, prepare, 0)

    def energy(position):
        return occ_ref[order_ref[position]]

    def compute(which, part):
        at = pl.ds(pl.multiple_of(part * STEP, STEP), STEP)
        partner = jnp.where(which == OWN, me, jnp.where(which == NEXT, after, jnp.where(which == PREV, before, opposite)))
        total = energy(me) + energy(partner)
        w = weight[which, 0:1]
        new_high, new_low = split(held[which, at])
        high[at], low[at] = new_high, new_low
        both = jnp.concatenate([new_high, new_low], axis=0)
        wide = nt(own_high[...], both)
        coupling = wide[:, :STEP] + wide[:, STEP:] + nt(own_low[...], new_high)
        mine = coupling / (total - virt_col[...] - virt_row[:, at])
        amp[:, at] = mine
        row = lax.broadcasted_iota(jnp.int32, (rows, STEP), 0)
        theirs = jnp.where(row < (part + 1) * STEP, amp[at].T, 0.0)
        tilde_high, tilde_low = split(w * (2.0 * mine - theirs))
        tilde_twice = jnp.concatenate([tilde_high, tilde_high], axis=1)
        turned_high, turned_low = split((w * jnp.where(row < part * STEP, mine, 0.0)).T)
        turned = jnp.concatenate([turned_high, turned_low], axis=0)

        def columns(tile, carry):
            over = pl.ds(pl.multiple_of(tile * TILE, TILE), TILE)
            near_high, near_low = high[at, over], low[at, over]
            out_ref[:, over] += nn(tilde_twice, jnp.concatenate([near_high, near_low], axis=0)) + nn(tilde_low, near_high)
            back = nn(turned, high[:, over])
            out_ref[at, over] -= back[:STEP] + back[STEP:] + nn(turned_high, low[:, over])
            return carry

        lax.fori_loop(0, depth // TILE, columns, 0)

    own_from, near_from = 3, 24
    stride = rounds - 1
    near_to = near_from + 2 * rounds

    def step(slot, carry):
        far_arrived(slot)

        @pl.when(slot + rounds < slots)
        def _():
            start_hop(slot + rounds)

        @pl.when((lax.rem(slot, stride) == 1) & (slot < hops * stride))
        def _():
            minor_hop(slot // stride)

        @pl.when((slot == slots - rounds) & moved(lax.rem(place + hops, ring)))
        def _():
            minor_any(hops - 1).wait_recv()

        @pl.when((slot < rounds) & first)
        def _():
            pass_copy(slot, NEXT, row_last).start()

        @pl.when((slot == 6) & upward)
        def _():
            over_parts(lambda part: near_copy(part, PREV, after).wait_recv())
            over_parts(lambda part: near_copy(part, NEXT, before).start())

        @pl.when((slot == 14) & upward)
        def _():
            over_parts(lambda part: near_copy(part, NEXT, before).wait_recv())
            weight_copy().start()

            @pl.when(last)
            def _():
                over_parts(lambda part: pass_copy(part, PREV, row_first).start())

            @pl.when(~last)
            def _():
                over_parts(lambda part: near_copy(part, PREV, after).start())

        @pl.when((slot == near_from) & ~upward)
        def _():
            over_parts(lambda part: near_copy(part, NEXT, before).wait_recv())
            over_parts(lambda part: near_copy(part, PREV, after).wait_recv())

        @pl.when(slot == near_from + rounds)
        def _():
            weight_copy().wait_recv()

        early = slot < own_from + rounds
        late = slot >= slots - rounds
        since = slot - near_from

        @pl.when((early & (slot >= own_from)) | ((since >= 0) & (slot < near_to)) | late)
        def _():
            which = jnp.where(early, OWN, jnp.where(late, FAR, NEXT + since // rounds))
            part = jnp.where(early, slot - own_from, jnp.where(late, slot - (slots - rounds), lax.rem(since, rounds)))
            compute(which, part)

        return carry

    @pl.when(~upward)
    def _():
        weight_copy().start()

    lax.fori_loop(0, slots, step, 0)

    def sent(slot, carry):
        far_sent(slot)
        return carry

    lax.fori_loop(0, slots, sent, 0)

    def minor_sent(hop, carry):
        @pl.when(moved(to_feeder(hop)))
        def _():
            minor_any(hop).wait_send()

        return carry

    lax.fori_loop(0, hops, minor_sent, 0)
    weight_copy().wait_send()

    @pl.when(first | last)
    def _():
        over_parts(lambda part: pass_copy(part, PREV, after).wait_send())

    @pl.when(~last)
    def _():
        over_parts(lambda part: near_copy(part, PREV, after).wait_send())

    @pl.when(~first)
    def _():
        over_parts(lambda part: near_copy(part, NEXT, before).wait_send())


def body(slices, occ_energy, virt_energy, order, near_keep, far_keep):
    n = lax.axis_size("orb")
    rows, depth = slices.shape[1:]
    hops = n // 2 // ROW
    rounds = rows // STEP
    vmem = pl.BlockSpec(memory_space=pltpu.VMEM)
    smem = pl.BlockSpec(memory_space=pltpu.SMEM)
    dma = pltpu.SemaphoreType.DMA
    density = pl.pallas_call(
        functools.partial(kernel, n),
        out_shape=jax.ShapeDtypeStruct((rows, depth), F32),
        in_specs=[pl.BlockSpec(memory_space=pl.ANY), smem, vmem, smem, smem, smem],
        out_specs=vmem,
        scratch_shapes=[
            pltpu.VMEM((hops - 1, rows, depth), F32),
            pltpu.VMEM((hops - 1, MINOR, depth), F32),
            pltpu.VMEM((4, rows, depth), F32),
            pltpu.VMEM((rows, depth), BF16),
            pltpu.VMEM((rows, depth), BF16),
            pltpu.VMEM((rows, depth), BF16),
            pltpu.VMEM((rows, depth), BF16),
            pltpu.VMEM((rows, rows), F32),
            pltpu.VMEM((rows, STEP), F32),
            pltpu.VMEM((1, rows), F32),
            pltpu.VMEM((4, 8, STEP), F32),
            dma((hops * rounds,)),
            dma((hops * rounds,)),
            dma((hops,)),
            dma((hops,)),
            dma((4, rounds)),
            dma((4, rounds)),
            dma((rounds,)),
            dma((2,)),
            dma,
        ],
        compiler_params=pltpu.CompilerParams(
            collective_id=0, has_side_effects=True, vmem_limit_bytes=62 * 1024 * 1024
        ),
    )(slices[0], occ_energy, virt_energy, order, near_keep, far_keep)
    return density[None]


def solution(mesh):
    return jax.shard_map(
        body,
        mesh=mesh,
        in_specs=(
            P(("frag", "orb"), None, None),
            P("frag"),
            P("frag"),
            P("frag"),
            P(("frag", "orb")),
            P("frag"),
        ),
        out_specs=P(("frag", "orb"), None, None),
        check_vma=False,
    )
```

```python
import functools

import jax
import jax.numpy as jnp
from jax import lax
from jax.experimental import pallas as pl
from jax.experimental.pallas import tpu as pltpu
from jax.sharding import PartitionSpec as P

MESH = pl.DeviceIdType.MESH
ROW = 8
CORES = 2
OWN, NEXT, PREV, FAR = range(4)
STEP = 128
TILE = 256
MINOR = 24
F32 = jnp.float32
BF16 = jnp.bfloat16


def split(x):
    high = x.astype(BF16)
    return high, (x - high.astype(F32)).astype(BF16)


def nt(left, right):
    return lax.dot_general(left, right, (((1,), (1,)), ((), ())), preferred_element_type=F32)


def nn(left, right):
    return jnp.dot(left, right, preferred_element_type=F32)


def kernel(
    n,
    own_ref, occ_hbm, virt_hbm, order_hbm, near_ref, far_hbm,
    out_ref,
    acc, occ_ref, virt_ref, order_ref, far_ref,
    transit, minor, held, own_high, own_low, high, low, amp, virt_col, virt_row, weight,
    send_sem, recv_sem, minor_send, minor_recv, near_send, near_recv, pass_send, weight_sem, load_sem, small_sem, out_sem,
):
    rows, depth = acc.shape
    rounds = rows // STEP
    middle = n // 2
    hops = middle // ROW
    slots = hops * rounds
    me = lax.axis_index("orb")
    inside = lax.rem(me, ROW)
    base = me - inside
    upward = lax.rem(inside, CORES) == 1
    above = lax.rem(me + ROW, n)
    below = lax.rem(me + n - ROW, n)
    onward = jnp.where(upward, above, below)
    feeder = jnp.where(upward, below, above)
    ring = n // ROW
    place = me // ROW
    after = lax.rem(me + 1, n)
    before = lax.rem(me + n - 1, n)
    opposite = lax.rem(me + middle, n)
    first = inside == 0
    last = inside == ROW - 1
    row_first, row_last = base, base + ROW - 1

    load = pltpu.make_async_copy(own_ref, held.at[OWN], load_sem)
    load.start()
    small = [
        pltpu.make_async_copy(src, dst, small_sem.at[i])
        for i, (src, dst) in enumerate(((occ_hbm, occ_ref), (virt_hbm, virt_ref), (order_hbm, order_ref), (far_hbm, far_ref)))
    ]
    for copy in small:
        copy.start()
    barrier = pltpu.get_barrier_semaphore()

    def greet(device):
        pl.semaphore_signal(barrier, inc=1, device_id={"orb": device}, device_id_type=MESH)

    greet(feeder)

    @pl.when(upward)
    def _():
        greet(before)
        greet(jnp.where(last, row_first, after))

    @pl.when(first)
    def _():
        greet(before)

    pl.semaphore_wait(barrier, jnp.where(upward, jnp.where(last, 2, 1), 3))
    load.wait()
    own = held.at[OWN]

    def remote(src, dst, send, recv, device):
        return pltpu.make_async_remote_copy(
            src_ref=src, dst_ref=dst, send_sem=send, recv_sem=recv,
            device_id={"orb": device}, device_id_type=MESH,
        )

    def band(part):
        return pl.ds(pl.multiple_of(part * STEP, STEP), STEP)

    def moved(source):
        return (source >= hops) == upward

    def from_feeder(distance):
        return lax.rem(place + jnp.where(upward, ring - distance, distance), ring)

    def to_feeder(distance):
        return lax.rem(place + jnp.where(upward, distance, ring - distance), ring)

    def on_chunk(hop, part, source, act):
        short = (hop > 0) & (part == 0) & moved(source)

        @pl.when(short)
        def _():
            act(pl.ds(MINOR, STEP - MINOR))

        @pl.when(~short)
        def _():
            act(band(part))

    def start_hop(slot):
        hop, part = slot // rounds, lax.rem(slot, rounds)
        sems = send_sem.at[slot], recv_sem.at[slot]

        def act(at):
            @pl.when(hop == 0)
            def _():
                remote(own.at[at], transit.at[0, at], *sems, onward).start()

            @pl.when((hop > 0) & (hop < hops - 1))
            def _():
                remote(transit.at[hop - 1, at], transit.at[hop, at], *sems, onward).start()

            @pl.when(hop == hops - 1)
            def _():
                remote(transit.at[hop - 1, at], held.at[FAR, at], *sems, onward).start()

        on_chunk(hop, part, from_feeder(hop), act)

    def far_copy(slot, at):
        return remote(own.at[at], transit.at[0, at], send_sem.at[slot], recv_sem.at[slot], onward)

    def far_arrived(slot):
        hop, part = slot // rounds, lax.rem(slot, rounds)
        on_chunk(hop, part, from_feeder(hop + 1), lambda at: far_copy(slot, at).wait_recv())

    def far_sent(slot):
        hop, part = slot // rounds, lax.rem(slot, rounds)
        on_chunk(hop, part, from_feeder(hop), lambda at: far_copy(slot, at).wait_send())

    few = pl.ds(0, MINOR)

    def minor_copy(hop, src, dst):
        return remote(src, dst, minor_send.at[hop], minor_recv.at[hop], feeder)

    def minor_any(hop):
        return minor_copy(hop, own.at[few], held.at[FAR, few])

    def minor_hop(hop):
        @pl.when(moved(to_feeder(hop)))
        def _():
            @pl.when(hop == 0)
            def _():
                minor_copy(hop, own.at[few], minor.at[0]).start()

            @pl.when(hop > 0)
            def _():
                minor_any(hop - 1).wait_recv()

            @pl.when((hop > 0) & (hop < hops - 1))
            def _():
                minor_copy(hop, minor.at[hop - 1], minor.at[hop]).start()

            @pl.when(hop == hops - 1)
            def _():
                minor_copy(hop, minor.at[hop - 1], held.at[FAR, few]).start()

    def near_copy(part, slot, device):
        at = band(part)
        return remote(own.at[at], held.at[slot, at], near_send.at[slot, part], near_recv.at[slot, part], device)

    def pass_copy(part, slot, device):
        at = band(part)
        return remote(transit.at[0, at], held.at[slot, at], pass_send.at[part], near_recv.at[slot, part], device)

    def weight_copy():
        return remote(weight.at[NEXT], weight.at[PREV], weight_sem.at[0], weight_sem.at[1], after)

    def over_parts(act):
        def one(part, carry):
            act(part)
            return carry

        lax.fori_loop(0, rounds, one, 0)

    over_parts(start_hop)

    @pl.when(~upward)
    def _():
        over_parts(lambda part: near_copy(part, PREV, after).start())

        @pl.when(~first)
        def _():
            over_parts(lambda part: near_copy(part, NEXT, before).start())

    for copy in small:
        copy.wait()
    weight[OWN] = jnp.ones(weight.shape[1:], F32)
    weight[NEXT] = jnp.full(weight.shape[1:], near_ref[0].astype(F32), F32)
    weight[FAR] = jnp.full(weight.shape[1:], far_ref[lax.rem(me, middle)].astype(F32), F32)
    virt_row[...] = virt_ref[...].reshape(1, rows)
    virt_col[...] = jnp.broadcast_to(virt_row[...], (STEP, rows)).T

    def prepare(part, carry):
        at = pl.ds(pl.multiple_of(part * STEP, STEP), STEP)
        own_high[at], own_low[at] = split(held[OWN, at])
        high[at] = jnp.zeros((STEP, depth), BF16)
        low[at] = jnp.zeros((STEP, depth), BF16)
        acc[at] = jnp.zeros((STEP, depth), F32)
        return carry

    lax.fori_loop(0, rounds, prepare, 0)

    def energy(position):
        return occ_ref[order_ref[position]]

    def compute(which, part, final=False):
        at = pl.ds(part * STEP, STEP) if final else band(part)
        partner = jnp.where(which == OWN, me, jnp.where(which == NEXT, after, jnp.where(which == PREV, before, opposite)))
        total = energy(me) + energy(partner)
        w = weight[which, 0:1]
        new_high, new_low = split(held[which, at])
        high[at], low[at] = new_high, new_low
        both = jnp.concatenate([new_high, new_low], axis=0)
        wide = nt(own_high[...], both)
        coupling = wide[:, :STEP] + wide[:, STEP:] + nt(own_low[...], new_high)
        mine = coupling / (total - virt_col[...] - virt_row[:, at])
        amp[:, at] = mine
        row = lax.broadcasted_iota(jnp.int32, (rows, STEP), 0)
        theirs = jnp.where(row < (part + 1) * STEP, amp[at].T, 0.0)
        tilde_high, tilde_low = split(w * (2.0 * mine - theirs))
        tilde_twice = jnp.concatenate([tilde_high, tilde_high], axis=1)
        turned_high, turned_low = split((w * jnp.where(row < part * STEP, mine, 0.0)).T)
        turned = jnp.concatenate([turned_high, turned_low], axis=0)

        def columns(over):
            near_high, near_low = high[at, over], low[at, over]
            acc[:, over] += nn(tilde_twice, jnp.concatenate([near_high, near_low], axis=0)) + nn(tilde_low, near_high)
            back = nn(turned, high[:, over])
            acc[at, over] -= back[:STEP] + back[STEP:] + nn(turned_high, low[:, over])

        if final:
            for tile in range(depth // TILE):
                columns(pl.ds(tile * TILE, TILE))
                if tile > 0:
                    write_out(tile - 1).start()
        else:

            def one(tile, carry):
                columns(pl.ds(pl.multiple_of(tile * TILE, TILE), TILE))
                return carry

            lax.fori_loop(0, depth // TILE, one, 0)

    def write_out(tile):
        over = pl.ds(tile * TILE, TILE)
        return pltpu.make_async_copy(acc.at[:, over], out_ref.at[:, over], out_sem.at[tile])

    own_from, near_from = 3, 24
    stride = rounds - 1
    near_to = near_from + 2 * rounds

    def step(slot, carry):
        far_arrived(slot)

        @pl.when(slot + rounds < slots)
        def _():
            start_hop(slot + rounds)

        @pl.when((lax.rem(slot, stride) == 1) & (slot < hops * stride))
        def _():
            minor_hop(slot // stride)

        @pl.when((slot == slots - rounds) & moved(lax.rem(place + hops, ring)))
        def _():
            minor_any(hops - 1).wait_recv()

        @pl.when((slot < rounds) & first)
        def _():
            pass_copy(slot, NEXT, row_last).start()

        @pl.when((slot == 6) & upward)
        def _():
            over_parts(lambda part: near_copy(part, PREV, after).wait_recv())
            over_parts(lambda part: near_copy(part, NEXT, before).start())

        @pl.when((slot == 14) & upward)
        def _():
            over_parts(lambda part: near_copy(part, NEXT, before).wait_recv())
            weight_copy().start()

            @pl.when(last)
            def _():
                over_parts(lambda part: pass_copy(part, PREV, row_first).start())

            @pl.when(~last)
            def _():
                over_parts(lambda part: near_copy(part, PREV, after).start())

        @pl.when((slot == near_from) & ~upward)
        def _():
            over_parts(lambda part: near_copy(part, NEXT, before).wait_recv())
            over_parts(lambda part: near_copy(part, PREV, after).wait_recv())

        @pl.when(slot == near_from + rounds)
        def _():
            weight_copy().wait_recv()

        early = slot < own_from + rounds
        late = slot >= slots - rounds
        since = slot - near_from

        @pl.when((early & (slot >= own_from)) | ((since >= 0) & (slot < near_to)) | late)
        def _():
            which = jnp.where(early, OWN, jnp.where(late, FAR, NEXT + since // rounds))
            part = jnp.where(early, slot - own_from, jnp.where(late, slot - (slots - rounds), lax.rem(since, rounds)))
            compute(which, part)

        return carry

    @pl.when(~upward)
    def _():
        weight_copy().start()

    lax.fori_loop(0, slots - 1, step, 0)
    far_arrived(slots - 1)
    compute(FAR, rounds - 1, final=True)

    def sent(slot, carry):
        far_sent(slot)
        return carry

    lax.fori_loop(0, slots, sent, 0)

    def minor_sent(hop, carry):
        @pl.when(moved(to_feeder(hop)))
        def _():
            minor_any(hop).wait_send()

        return carry

    lax.fori_loop(0, hops, minor_sent, 0)
    weight_copy().wait_send()

    @pl.when(first | last)
    def _():
        over_parts(lambda part: pass_copy(part, PREV, after).wait_send())

    @pl.when(~last)
    def _():
        over_parts(lambda part: near_copy(part, PREV, after).wait_send())

    @pl.when(~first)
    def _():
        over_parts(lambda part: near_copy(part, NEXT, before).wait_send())

    tiles = depth // TILE
    write_out(tiles - 1).start()
    for tile in range(tiles):
        write_out(tile).wait()


def settle(src_ref, dst_ref, bands, in_sem, out_sem):
    count, size = bands.shape[:2]
    arrive = [pltpu.make_async_copy(src_ref.at[pl.ds(i * size, size)], bands.at[i], in_sem.at[i]) for i in range(count)]
    leave = [pltpu.make_async_copy(bands.at[i], dst_ref.at[pl.ds(i * size, size)], out_sem.at[i]) for i in range(count)]
    for copy in arrive:
        copy.start()
    for come, go in zip(arrive, leave):
        come.wait()
        go.start()
    for copy in leave:
        copy.wait()


def body(slices, occ_energy, virt_energy, order, near_keep, far_keep):
    n = lax.axis_size("orb")
    rows, depth = slices.shape[1:]
    hops = n // 2 // ROW
    rounds = rows // STEP
    anywhere = pl.BlockSpec(memory_space=pl.ANY)
    smem = pl.BlockSpec(memory_space=pltpu.SMEM)
    dma = pltpu.SemaphoreType.DMA
    density = pl.pallas_call(
        functools.partial(kernel, n),
        out_shape=jax.ShapeDtypeStruct((rows, depth), F32),
        in_specs=[anywhere, anywhere, anywhere, anywhere, smem, anywhere],
        out_specs=anywhere,
        scratch_shapes=[
            pltpu.VMEM((rows, depth), F32),
            pltpu.SMEM(occ_energy.shape, F32),
            pltpu.VMEM(virt_energy.shape, F32),
            pltpu.SMEM(order.shape, jnp.int32),
            pltpu.SMEM(far_keep.shape, jnp.int32),
            pltpu.VMEM((hops - 1, rows, depth), F32),
            pltpu.VMEM((hops - 1, MINOR, depth), F32),
            pltpu.VMEM((4, rows, depth), F32),
            pltpu.VMEM((rows, depth), BF16),
            pltpu.VMEM((rows, depth), BF16),
            pltpu.VMEM((rows, depth), BF16),
            pltpu.VMEM((rows, depth), BF16),
            pltpu.VMEM((rows, rows), F32),
            pltpu.VMEM((rows, STEP), F32),
            pltpu.VMEM((1, rows), F32),
            pltpu.VMEM((4, 8, STEP), F32),
            dma((hops * rounds,)),
            dma((hops * rounds,)),
            dma((hops,)),
            dma((hops,)),
            dma((4, rounds)),
            dma((4, rounds)),
            dma((rounds,)),
            dma((2,)),
            dma,
            dma((4,)),
            dma((depth // TILE,)),
        ],
        compiler_params=pltpu.CompilerParams(
            collective_id=0, has_side_effects=True, vmem_limit_bytes=62 * 1024 * 1024
        ),
    )(slices[0], occ_energy, virt_energy, order, near_keep, far_keep)
    density = pl.pallas_call(
        settle,
        out_shape=jax.ShapeDtypeStruct((rows, depth), F32),
        in_specs=[anywhere],
        out_specs=anywhere,
        scratch_shapes=[pltpu.VMEM((rounds, STEP, depth), F32), dma((rounds,)), dma((rounds,))],
    )(density)
    return density[None]


def solution(mesh):
    return jax.shard_map(
        body,
        mesh=mesh,
        in_specs=(
            P(("frag", "orb"), None, None),
            P("frag"),
            P("frag"),
            P("frag"),
            P(("frag", "orb")),
            P("frag"),
        ),
        out_specs=P(("frag", "orb"), None, None),
        check_vma=False,
    )
```

```python
import functools

import jax
import jax.numpy as jnp
from jax import lax
from jax.experimental import pallas as pl
from jax.experimental.pallas import tpu as pltpu
from jax.sharding import PartitionSpec as P

MESH = pl.DeviceIdType.MESH
ROW = 8
CORES = 2
OWN, NEXT, PREV, FAR = range(4)
STEP = 128
TILE = 256
MINOR = 16
F32 = jnp.float32
BF16 = jnp.bfloat16


def split(x):
    high = x.astype(BF16)
    return high, (x - high.astype(F32)).astype(BF16)


def nt(left, right):
    return lax.dot_general(left, right, (((1,), (1,)), ((), ())), preferred_element_type=F32)


def nn(left, right):
    return jnp.dot(left, right, preferred_element_type=F32)


def kernel(
    n,
    own_ref, occ_hbm, virt_hbm, order_hbm, near_ref, far_hbm,
    out_ref,
    acc, occ_ref, virt_ref, order_ref, far_ref,
    transit, minor, held, own_high, own_low, high, low, amp, virt_col, virt_row, weight,
    send_sem, recv_sem, minor_send, minor_recv, near_send, near_recv, pass_send, weight_sem, load_sem, small_sem, out_sem,
):
    rows, depth = acc.shape
    rounds = rows // STEP
    middle = n // 2
    hops = middle // ROW
    slots = hops * rounds
    me = lax.axis_index("orb")
    inside = lax.rem(me, ROW)
    base = me - inside
    upward = lax.rem(inside, CORES) == 1
    above = lax.rem(me + ROW, n)
    below = lax.rem(me + n - ROW, n)
    onward = jnp.where(upward, above, below)
    feeder = jnp.where(upward, below, above)
    ring = n // ROW
    place = me // ROW
    after = lax.rem(me + 1, n)
    before = lax.rem(me + n - 1, n)
    opposite = lax.rem(me + middle, n)
    first = inside == 0
    last = inside == ROW - 1
    row_first, row_last = base, base + ROW - 1

    load = pltpu.make_async_copy(own_ref, held.at[OWN], load_sem)
    load.start()
    small = [
        pltpu.make_async_copy(src, dst, small_sem.at[i])
        for i, (src, dst) in enumerate(((occ_hbm, occ_ref), (virt_hbm, virt_ref), (order_hbm, order_ref), (far_hbm, far_ref)))
    ]
    for copy in small:
        copy.start()
    barrier = pltpu.get_barrier_semaphore()

    def greet(device):
        pl.semaphore_signal(barrier, inc=1, device_id={"orb": device}, device_id_type=MESH)

    greet(feeder)

    @pl.when(upward)
    def _():
        greet(before)
        greet(jnp.where(last, row_first, after))

    @pl.when(first)
    def _():
        greet(before)

    closing = upward & (place == ring - 1)

    @pl.when(upward & (place == hops - 2))
    def _():
        greet(lax.rem(me + (ring - hops + 1) * ROW, n))

    heard = jnp.where(upward, jnp.where(last, 2, 1), 3) + jnp.where(closing, 1, 0)
    pl.semaphore_wait(barrier, heard)
    load.wait()
    own = held.at[OWN]

    def remote(src, dst, send, recv, device):
        return pltpu.make_async_remote_copy(
            src_ref=src, dst_ref=dst, send_sem=send, recv_sem=recv,
            device_id={"orb": device}, device_id_type=MESH,
        )

    def band(part):
        return pl.ds(pl.multiple_of(part * STEP, STEP), STEP)

    def moved(source):
        return (source >= hops) == upward

    def from_feeder(distance):
        return lax.rem(place + jnp.where(upward, ring - distance, distance), ring)

    def to_feeder(distance):
        return lax.rem(place + jnp.where(upward, distance, ring - distance), ring)

    def on_chunk(hop, part, source, act):
        short = (hop > 0) & (part == 0) & moved(source)

        @pl.when(short)
        def _():
            act(pl.ds(MINOR, STEP - MINOR))

        @pl.when(~short)
        def _():
            act(band(part))

    def start_hop(slot):
        hop, part = slot // rounds, lax.rem(slot, rounds)
        sems = send_sem.at[slot], recv_sem.at[slot]

        def act(at):
            @pl.when(hop == 0)
            def _():
                remote(own.at[at], transit.at[0, at], *sems, onward).start()

            @pl.when((hop > 0) & (hop < hops - 1))
            def _():
                remote(transit.at[hop - 1, at], transit.at[hop, at], *sems, onward).start()

            @pl.when(hop == hops - 1)
            def _():
                remote(transit.at[hop - 1, at], held.at[FAR, at], *sems, onward).start()

        on_chunk(hop, part, from_feeder(hop), act)

    def late_chunk(slot, source):
        return upward & (lax.rem(slot, rounds) == rounds - 1) & (source == ring - 2)

    def not_sent(slot):
        hop = slot // rounds
        return late_chunk(slot, from_feeder(hop)) & (hop > 1)

    def not_received(slot):
        hop = slot // rounds
        return late_chunk(slot, from_feeder(hop + 1)) & (hop > 0) & (hop < hops - 1)

    held_back = 2 * rounds - 1

    def late_copy():
        at = pl.ds(rows - STEP, STEP)
        target = lax.rem(me + (hops - 1) * ROW, n)
        return remote(transit.at[0, at], held.at[FAR, at], send_sem.at[held_back], recv_sem.at[slots - 1], target)

    def far_copy(slot, at):
        return remote(own.at[at], transit.at[0, at], send_sem.at[slot], recv_sem.at[slot], onward)

    def far_arrived(slot):
        hop, part = slot // rounds, lax.rem(slot, rounds)
        on_chunk(hop, part, from_feeder(hop + 1), lambda at: far_copy(slot, at).wait_recv())

    def far_sent(slot):
        hop, part = slot // rounds, lax.rem(slot, rounds)
        on_chunk(hop, part, from_feeder(hop), lambda at: far_copy(slot, at).wait_send())

    few = pl.ds(0, MINOR)

    def minor_copy(hop, src, dst):
        return remote(src, dst, minor_send.at[hop], minor_recv.at[hop], feeder)

    def minor_any(hop):
        return minor_copy(hop, own.at[few], held.at[FAR, few])

    def minor_hop(hop):
        @pl.when(moved(to_feeder(hop)))
        def _():
            @pl.when(hop == 0)
            def _():
                minor_copy(hop, own.at[few], minor.at[0]).start()

            @pl.when(hop > 0)
            def _():
                minor_any(hop - 1).wait_recv()

            @pl.when((hop > 0) & (hop < hops - 1))
            def _():
                minor_copy(hop, minor.at[hop - 1], minor.at[hop]).start()

            @pl.when(hop == hops - 1)
            def _():
                minor_copy(hop, minor.at[hop - 1], held.at[FAR, few]).start()

    def near_copy(part, slot, device):
        at = band(part)
        return remote(own.at[at], held.at[slot, at], near_send.at[slot, part], near_recv.at[slot, part], device)

    def pass_copy(part, slot, device):
        at = band(part)
        return remote(transit.at[0, at], held.at[slot, at], pass_send.at[part], near_recv.at[slot, part], device)

    def weight_copy():
        return remote(weight.at[NEXT], weight.at[PREV], weight_sem.at[0], weight_sem.at[1], after)

    def over_parts(act):
        def one(part, carry):
            act(part)
            return carry

        lax.fori_loop(0, rounds, one, 0)

    over_parts(start_hop)

    @pl.when(~upward)
    def _():
        over_parts(lambda part: near_copy(part, PREV, after).start())

        @pl.when(~first)
        def _():
            over_parts(lambda part: near_copy(part, NEXT, before).start())

    for copy in small:
        copy.wait()
    weight[OWN] = jnp.ones(weight.shape[1:], F32)
    weight[NEXT] = jnp.full(weight.shape[1:], near_ref[0].astype(F32), F32)
    weight[FAR] = jnp.full(weight.shape[1:], far_ref[lax.rem(me, middle)].astype(F32), F32)
    virt_row[...] = virt_ref[...].reshape(1, rows)
    virt_col[...] = jnp.broadcast_to(virt_row[...], (STEP, rows)).T

    def prepare(part, carry):
        at = pl.ds(pl.multiple_of(part * STEP, STEP), STEP)
        own_high[at], own_low[at] = split(held[OWN, at])
        high[at] = jnp.zeros((STEP, depth), BF16)
        low[at] = jnp.zeros((STEP, depth), BF16)
        acc[at] = jnp.zeros((STEP, depth), F32)
        return carry

    lax.fori_loop(0, rounds, prepare, 0)

    def energy(position):
        return occ_ref[order_ref[position]]

    def compute(which, part, final=False):
        at = pl.ds(part * STEP, STEP) if final else band(part)
        partner = jnp.where(which == OWN, me, jnp.where(which == NEXT, after, jnp.where(which == PREV, before, opposite)))
        total = energy(me) + energy(partner)
        w = weight[which, 0:1]
        new_high, new_low = split(held[which, at])
        high[at], low[at] = new_high, new_low
        both = jnp.concatenate([new_high, new_low], axis=0)
        wide = nt(own_high[...], both)
        coupling = wide[:, :STEP] + wide[:, STEP:] + nt(own_low[...], new_high)
        mine = coupling / (total - virt_col[...] - virt_row[:, at])
        amp[:, at] = mine
        row = lax.broadcasted_iota(jnp.int32, (rows, STEP), 0)
        theirs = jnp.where(row < (part + 1) * STEP, amp[at].T, 0.0)
        tilde_high, tilde_low = split(w * (2.0 * mine - theirs))
        tilde_twice = jnp.concatenate([tilde_high, tilde_high], axis=1)
        turned_high, turned_low = split((w * jnp.where(row < part * STEP, mine, 0.0)).T)
        turned = jnp.concatenate([turned_high, turned_low], axis=0)

        def columns(over):
            near_high, near_low = high[at, over], low[at, over]
            acc[:, over] += nn(tilde_twice, jnp.concatenate([near_high, near_low], axis=0)) + nn(tilde_low, near_high)
            back = nn(turned, high[:, over])
            acc[at, over] -= back[:STEP] + back[STEP:] + nn(turned_high, low[:, over])

        if final:
            for tile in range(depth // TILE):
                columns(pl.ds(tile * TILE, TILE))
                if tile > 0:
                    write_out(tile - 1).start()
        else:

            def one(tile, carry):
                columns(pl.ds(pl.multiple_of(tile * TILE, TILE), TILE))
                return carry

            lax.fori_loop(0, depth // TILE, one, 0)

    def write_out(tile):
        over = pl.ds(tile * TILE, TILE)
        return pltpu.make_async_copy(acc.at[:, over], out_ref.at[:, over], out_sem.at[tile])

    own_from, near_from = 3, 24
    stride = rounds - 1
    near_to = near_from + 2 * rounds

    def step(slot, carry):
        @pl.when(~not_received(slot))
        def _():
            far_arrived(slot)

        later = slot + rounds

        @pl.when((later < slots) & ~not_sent(later) & ~(closing & (later == held_back)))
        def _():
            start_hop(later)

        @pl.when(closing & (later == slots - 1))
        def _():
            late_copy().start()

        @pl.when((lax.rem(slot, stride) == 1) & (slot < hops * stride))
        def _():
            minor_hop(slot // stride)

        @pl.when((slot == slots - rounds) & moved(lax.rem(place + hops, ring)))
        def _():
            minor_any(hops - 1).wait_recv()

        @pl.when((slot < rounds) & first)
        def _():
            pass_copy(slot, NEXT, row_last).start()

        @pl.when((slot == 6) & upward)
        def _():
            over_parts(lambda part: near_copy(part, PREV, after).wait_recv())
            over_parts(lambda part: near_copy(part, NEXT, before).start())

        @pl.when((slot == 14) & upward)
        def _():
            over_parts(lambda part: near_copy(part, NEXT, before).wait_recv())
            weight_copy().start()

            @pl.when(last)
            def _():
                over_parts(lambda part: pass_copy(part, PREV, row_first).start())

            @pl.when(~last)
            def _():
                over_parts(lambda part: near_copy(part, PREV, after).start())

        @pl.when((slot == near_from) & ~upward)
        def _():
            over_parts(lambda part: near_copy(part, NEXT, before).wait_recv())
            over_parts(lambda part: near_copy(part, PREV, after).wait_recv())

        @pl.when(slot == near_from + rounds)
        def _():
            weight_copy().wait_recv()

        early = slot < own_from + rounds
        late = slot >= slots - rounds
        since = slot - near_from

        @pl.when((early & (slot >= own_from)) | ((since >= 0) & (slot < near_to)) | late)
        def _():
            which = jnp.where(early, OWN, jnp.where(late, FAR, NEXT + since // rounds))
            part = jnp.where(early, slot - own_from, jnp.where(late, slot - (slots - rounds), lax.rem(since, rounds)))
            compute(which, part)

        return carry

    @pl.when(~upward)
    def _():
        weight_copy().start()

    lax.fori_loop(0, slots - 1, step, 0)
    far_arrived(slots - 1)
    compute(FAR, rounds - 1, final=True)

    def sent(slot, carry):
        @pl.when(~not_sent(slot))
        def _():
            far_sent(slot)

        return carry

    lax.fori_loop(0, slots, sent, 0)

    def minor_sent(hop, carry):
        @pl.when(moved(to_feeder(hop)))
        def _():
            minor_any(hop).wait_send()

        return carry

    lax.fori_loop(0, hops, minor_sent, 0)
    weight_copy().wait_send()

    @pl.when(first | last)
    def _():
        over_parts(lambda part: pass_copy(part, PREV, after).wait_send())

    @pl.when(~last)
    def _():
        over_parts(lambda part: near_copy(part, PREV, after).wait_send())

    @pl.when(~first)
    def _():
        over_parts(lambda part: near_copy(part, NEXT, before).wait_send())

    tiles = depth // TILE
    write_out(tiles - 1).start()
    for tile in range(tiles):
        write_out(tile).wait()


def settle(src_ref, dst_ref, bands, in_sem, out_sem):
    count, size = bands.shape[:2]
    arrive = [pltpu.make_async_copy(src_ref.at[pl.ds(i * size, size)], bands.at[i], in_sem.at[i]) for i in range(count)]
    leave = [pltpu.make_async_copy(bands.at[i], dst_ref.at[pl.ds(i * size, size)], out_sem.at[i]) for i in range(count)]
    for copy in arrive:
        copy.start()
    for come, go in zip(arrive, leave):
        come.wait()
        go.start()
    for copy in leave:
        copy.wait()


def body(slices, occ_energy, virt_energy, order, near_keep, far_keep):
    n = lax.axis_size("orb")
    rows, depth = slices.shape[1:]
    hops = n // 2 // ROW
    rounds = rows // STEP
    anywhere = pl.BlockSpec(memory_space=pl.ANY)
    smem = pl.BlockSpec(memory_space=pltpu.SMEM)
    dma = pltpu.SemaphoreType.DMA
    density = pl.pallas_call(
        functools.partial(kernel, n),
        out_shape=jax.ShapeDtypeStruct((rows, depth), F32),
        in_specs=[anywhere, anywhere, anywhere, anywhere, smem, anywhere],
        out_specs=anywhere,
        scratch_shapes=[
            pltpu.VMEM((rows, depth), F32),
            pltpu.SMEM(occ_energy.shape, F32),
            pltpu.VMEM(virt_energy.shape, F32),
            pltpu.SMEM(order.shape, jnp.int32),
            pltpu.SMEM(far_keep.shape, jnp.int32),
            pltpu.VMEM((hops - 1, rows, depth), F32),
            pltpu.VMEM((hops - 1, MINOR, depth), F32),
            pltpu.VMEM((4, rows, depth), F32),
            pltpu.VMEM((rows, depth), BF16),
            pltpu.VMEM((rows, depth), BF16),
            pltpu.VMEM((rows, depth), BF16),
            pltpu.VMEM((rows, depth), BF16),
            pltpu.VMEM((rows, rows), F32),
            pltpu.VMEM((rows, STEP), F32),
            pltpu.VMEM((1, rows), F32),
            pltpu.VMEM((4, 8, STEP), F32),
            dma((hops * rounds,)),
            dma((hops * rounds,)),
            dma((hops,)),
            dma((hops,)),
            dma((4, rounds)),
            dma((4, rounds)),
            dma((rounds,)),
            dma((2,)),
            dma,
            dma((4,)),
            dma((depth // TILE,)),
        ],
        compiler_params=pltpu.CompilerParams(
            collective_id=0, has_side_effects=True, vmem_limit_bytes=62 * 1024 * 1024
        ),
    )(slices[0], occ_energy, virt_energy, order, near_keep, far_keep)
    density = pl.pallas_call(
        settle,
        out_shape=jax.ShapeDtypeStruct((rows, depth), F32),
        in_specs=[anywhere],
        out_specs=anywhere,
        scratch_shapes=[pltpu.VMEM((rounds, STEP, depth), F32), dma((rounds,)), dma((rounds,))],
    )(density)
    return density[None]


def solution(mesh):
    return jax.shard_map(
        body,
        mesh=mesh,
        in_specs=(
            P(("frag", "orb"), None, None),
            P("frag"),
            P("frag"),
            P("frag"),
            P(("frag", "orb")),
            P("frag"),
        ),
        out_specs=P(("frag", "orb"), None, None),
        check_vma=False,
    )
```
